128 devices in a mesh: ctx: 32 (over y, z, core), head: 4 (over x).
Axes of the slice: x: 4, y: 4, z: 4, core: 2. Of those that a mesh axis runs over, the one named last changes fastest.
Arguments:
- query: bfloat16 [65536, 2048], P('ctx', 'head'), may hold values from -6 to 6
- key: bfloat16 [65536, 2048], P('ctx', 'head'), may hold values from -6 to 6
- value: bfloat16 [65536, 2048], P('ctx', 'head'), may hold values from -6 to 6
- gain: bfloat16 [2048], P('head'), may hold values from 0.099609375 to 1.8984375
- w_out: bfloat16 [2048, 2048], replicated, may hold values from -0.125 to 0.125
- d_out: bfloat16 [65536, 2048], P(('ctx', 'head')), may hold values from -6 to 6
Outputs:
- out: bfloat16 [65536, 2048], P(('ctx', 'head'))
- grad_query: bfloat16 [65536, 2048], P('ctx', 'head')
- grad_key: bfloat16 [65536, 2048], P('ctx', 'head')
- grad_value: bfloat16 [65536, 2048], P('ctx', 'head')
The draws below stay inside these ranges and needn't reach their ends.
All inputs are finite; a program needn't handle non-finite values.
Results may differ from the reference program's by a relative error of at most 0.018.
Values may be sent and summed in bfloat16 or wider, within the bound.
A program may use at most 128 MiB of HBM per device.

```python
import jax
import jax.numpy as jnp
from jax import lax

HEADS = 16
HDIM = 128
BLOCK = 128
D = 2048
TOKENS = 65536


def shard_levels(stream_key, shape, shards, low, largest):
    loudness = 1.0
    for axis_at, blocks in shards:
        steps = jax.random.uniform(jax.random.fold_in(jax.random.fold_in(stream_key, 6), axis_at), (blocks,), jnp.float32, low / len(shards), largest / len(shards))
        loudness = loudness * jnp.repeat(jnp.exp(steps), shape[axis_at] // blocks).reshape((-1,) + (1,) * (len(shape) - 1 - axis_at))
    return loudness


def centred(key, extent, scale, limit, pieces=(), kind=jnp.bfloat16):
    drawn = scale * jax.random.normal(key, extent, jnp.float32)
    if pieces:
        drawn = drawn * shard_levels(key, extent, pieces, -0.22, 0.18)
    return jnp.clip(drawn, -limit, limit).astype(kind)


def setup_inputs(seed: int = 0) -> dict:
    keys = jax.random.split(jax.random.key(seed), 7)
    return {
        "query": centred(keys[0], (TOKENS, D), 1.0, 6.0, ((0, 32), (1, 4))),
        "key": centred(keys[1], (TOKENS, D), 1.0, 6.0, ((0, 32), (1, 4))),
        "value": centred(keys[2], (TOKENS, D), 1.0, 6.0, ((0, 32), (1, 4))),
        "gain": jnp.clip(1.0 + 0.18 * jax.random.normal(keys[3], (D,), jnp.float32), 0.099609375, 1.8984375).astype(jnp.bfloat16),
        "w_out": centred(keys[4], (D, D), D ** -0.5, 0.125),
        "d_out": centred(keys[5], (TOKENS, D), 1.0, 6.0, ((0, 128),)),
    }


epsilon = 1e-06
highest = lax.Precision.HIGHEST

def rounded(values):
    return lax.optimization_barrier(values.astype(jnp.bfloat16)).astype(values.dtype)

def product(form, left, right):
    return jnp.einsum(form, left, right, precision=highest)

def reference(query, key, value, gain, w_out, d_out):
    nblocks = TOKENS // BLOCK
    causal = jnp.tril(jnp.ones((BLOCK, BLOCK), dtype=bool))[None]

    def split_blocks(array):
        return array.reshape(nblocks, BLOCK, HEADS, HDIM)

    def masked(scores):
        return rounded(jnp.where(causal, scores, jnp.zeros_like(scores)))
    inputs = (split_blocks(query), split_blocks(key), split_blocks(value))
    zero_state = jnp.zeros((HEADS, HDIM, HDIM), jnp.float32)

    def forward_step(state, block_in):
        q_blk, k_blk, v_blk = [piece.astype(jnp.float32) for piece in block_in]
        weights = masked(product('she,the->hst', q_blk, k_blk))
        output = product('hst,thf->shf', weights, v_blk) + product('she,hef->shf', q_blk, rounded(state))
        return (state + product('she,shf->hef', k_blk, v_blk), output)
    _, attended = lax.scan(forward_step, zero_state, inputs)
    attended = attended.reshape(TOKENS, HEADS, HDIM)
    inverse = lax.rsqrt(lax.optimization_barrier(jnp.mean(attended * attended, axis=-1, keepdims=True)) + epsilon)
    unit = attended * inverse
    scales = gain.astype(jnp.float32).reshape(HEADS, HDIM)
    normed = (unit * scales).astype(jnp.bfloat16).reshape(TOKENS, D)
    out = jnp.dot(normed, w_out, preferred_element_type=jnp.float32).astype(jnp.bfloat16)
    grad_rows = lax.dot_general(d_out, w_out, (((1,), (1,)), ((), ())), preferred_element_type=jnp.float32)
    grad_normed = rounded(grad_rows).reshape(TOKENS, HEADS, HDIM)
    grad_unit = grad_normed * scales
    grad_attended = inverse * (grad_unit - unit * lax.optimization_barrier(jnp.mean(grad_unit * unit, axis=-1, keepdims=True)))
    grad_blocks = split_blocks(grad_attended.astype(jnp.bfloat16))

    def query_step(state, block_in):
        k_blk, v_blk, g_blk = [piece.astype(jnp.float32) for piece in block_in]
        weights = masked(product('shf,thf->hst', g_blk, v_blk))
        grad_q = product('hst,the->she', weights, k_blk) + product('shf,hef->she', g_blk, rounded(state))
        return (state + product('she,shf->hef', k_blk, v_blk), grad_q)
    _, grad_query = lax.scan(query_step, zero_state, (inputs[1], inputs[2], grad_blocks))

    def key_step(later, block_in):
        q_blk, k_blk, v_blk, g_blk = [piece.astype(jnp.float32) for piece in block_in]
        weights = masked(product('shf,thf->hst', g_blk, v_blk))
        scores = masked(product('she,the->hst', q_blk, k_blk))
        frozen = rounded(later)
        grad_k = product('hst,she->the', weights, q_blk) + product('thf,hef->the', v_blk, frozen)
        grad_v = product('hst,shf->thf', scores, g_blk) + product('the,hef->thf', k_blk, frozen)
        return (later + product('she,shf->hef', q_blk, g_blk), (grad_k, grad_v))
    _, (grad_key, grad_value) = lax.scan(key_step, zero_state, inputs + (grad_blocks,), reverse=True)
    return (out, grad_query.reshape(TOKENS, D).astype(jnp.bfloat16), grad_key.reshape(TOKENS, D).astype(jnp.bfloat16), grad_value.reshape(TOKENS, D).astype(jnp.bfloat16))
```

```python
import jax
import jax.numpy as jnp
from jax import lax
from jax.experimental import pallas as pl
from jax.experimental.pallas import tpu as pltpu
from jax.sharding import PartitionSpec as P

HDIM = 128
BLOCK = 128
EPSILON = 1e-06
MESH = pl.DeviceIdType.MESH
F32 = jnp.float32
BF16 = jnp.bfloat16


def rows_of(index, size):
    return pl.ds(pl.multiple_of(index * size, size), size)


def dot_nn(a, b):
    return jnp.dot(a, b, preferred_element_type=F32)


def dot_nt(a, b):
    return lax.dot_general(a, b, (((1,), (1,)), ((), ())), preferred_element_type=F32)


def dot_tn(a, b):
    return lax.dot_general(a, b, (((0,), (0,)), ((), ())), preferred_element_type=F32)


def kernel(
    query, key, value, gain, w_out, d_out,
    out, grad_query, grad_key, grad_value,
    q, k, v, w, d, gn_send, gn, nm, nr, sc, gsc, g, pb, st, bg, unit, inv, sq, sk, sv, so,
    tb, ra, ea, rs, rb, pc, rc,
    load_sem, w_sem, gn_ssem, gn_rsem, nm_ssem, nm_rsem,
    a_ssem, a_rsem, b_ssem, b_rsem, c_ssem, c_rsem, gq_sem, gk_sem, gv_sem, out_sem,
):
    ci = lax.axis_index("ctx")
    hi = lax.axis_index("head")
    y = ci // 8
    me = lax.rem(ci, 8)
    heads = 4
    nblocks = 16

    pltpu.make_async_copy(d_out, d, load_sem.at[0]).start()

    def w_load(i):
        h = lax.rem(hi + (1 + 2 * i - 3 * (i // 2)) * (1 - i // 3), 4)
        return pltpu.make_async_copy(
            w_out.at[rows_of(h, 512), :], w.at[rows_of(h, 512), :], w_sem.at[i]
        )

    for i in range(4):
        w_load(i).start()
    loads = (
        pltpu.make_async_copy(key, k, load_sem.at[1]),
        pltpu.make_async_copy(value, v, load_sem.at[2]),
        pltpu.make_async_copy(query, q, load_sem.at[3]),
    )
    for load in loads:
        load.start()

    def near(i):
        return {"ctx": y * 8 + lax.rem(me + i, 8)}

    def far(i):
        return {"ctx": lax.rem(y + i, 4) * 8 + me}

    def across(o):
        return {"head": lax.rem(hi + o, 4)}

    barrier = pltpu.get_barrier_semaphore()
    for peer in (
        [across(o) for o in (1, 2, 3)]
        + [near(i) for i in range(1, 8)]
        + [far(i) for i in range(1, 4)]
    ):
        pl.semaphore_signal(barrier, inc=1, device_id=peer, device_id_type=MESH)
    pl.semaphore_wait(barrier, 13)

    def offset(j):
        return 1 + 2 * j - 3 * (j // 2)

    def gn_copy(j, half):
        return pltpu.make_async_remote_copy(
            src_ref=gn_send.at[j, rows_of(half, 256), :],
            dst_ref=gn.at[rows_of(hi * 2 + half, 256), :],
            send_sem=gn_ssem.at[j, half],
            recv_sem=gn_rsem.at[j, half],
            device_id=across(offset(j)),
            device_id_type=MESH,
        )

    def gn_arrival(j, half):
        source = lax.rem(hi - offset(j) + 4, 4)
        return pltpu.make_async_remote_copy(
            src_ref=gn_send.at[j, rows_of(half, 256), :],
            dst_ref=gn.at[rows_of(source * 2 + half, 256), :],
            send_sem=gn_ssem.at[j, half],
            recv_sem=gn_rsem.at[j, half],
            device_id=across(offset(j)),
            device_id_type=MESH,
        )

    pltpu.make_async_copy(d_out, d, load_sem.at[0]).wait()

    def gn_step(i, carry):
        half, j = i // 3, lax.rem(i, 3)

        @pl.when(half == 0)
        def _():
            w_load(j).wait()

        h = lax.rem(hi + offset(j), 4)
        gn_send[j, rows_of(half, 256), :] = dot_nt(
            d[rows_of(half, 256), :], w[rows_of(h, 512), :]
        ).astype(BF16)
        gn_copy(j, half).start()
        return carry

    lax.fori_loop(0, 6, gn_step, 0)

    loads[0].wait()
    loads[1].wait()
    st[0] = jnp.zeros((heads, HDIM, HDIM), F32)

    def state_step(b, carry):
        rows = rows_of(b, BLOCK)
        for h in range(heads):
            cols = slice(h * HDIM, (h + 1) * HDIM)
            st[b + 1, h] = st[b, h] + dot_tn(k[rows, cols], v[rows, cols])
        return carry

    lax.fori_loop(0, nblocks, state_step, 0)

    def a_copy(way, i, slot):
        return pltpu.make_async_remote_copy(
            src_ref=tb.at[way, rows_of(lax.rem(me + i, 8), 64), :],
            dst_ref=ra.at[way, slot],
            send_sem=a_ssem.at[way, i - 1],
            recv_sem=a_rsem.at[way, i - 1],
            device_id=near(i),
            device_id_type=MESH,
        )

    def b_copy(way, i, slot):
        return pltpu.make_async_remote_copy(
            src_ref=rs.at[way],
            dst_ref=rb.at[way, slot],
            send_sem=b_ssem.at[way, i - 1],
            recv_sem=b_rsem.at[way, i - 1],
            device_id=far(i),
            device_id_type=MESH,
        )

    def c_copy(way, i, slot):
        return pltpu.make_async_remote_copy(
            src_ref=pc.at[way, lax.rem(me + i, 8)],
            dst_ref=rc.at[way, rows_of(slot, 64), :],
            send_sem=c_ssem.at[way, i - 1],
            recv_sem=c_rsem.at[way, i - 1],
            device_id=near(i),
            device_id_type=MESH,
        )

    def exchange_a(way, total):
        tb[way] = total.reshape(heads * HDIM, HDIM).astype(BF16)
        ra[way, me] = tb[way, rows_of(me, 64), :]
        for i in range(1, 8):
            a_copy(way, i, me).start()

    def exchange_b(way):
        for i in range(1, 8):
            a_copy(way, i, lax.rem(me - i + 8, 8)).wait()
        run = jnp.zeros((64, HDIM), F32)
        for s in reversed(range(8)) if way else range(8):
            ea[way, s] = run
            run = run + ra[way, s].astype(F32)
        rs[way] = run
        rb[way, y] = jnp.zeros((64, HDIM), F32)
        for i in range(1, 4):
            b_copy(way, i, y).start()

    def exchange_c(way):
        for i in range(1, 4):
            b_copy(way, i, lax.rem(y - i + 4, 4)).wait()
        base = jnp.zeros((64, HDIM), F32)
        for s in range(4):
            passed = s > y if way else s < y
            base = base + jnp.where(passed, rb[way, s], jnp.zeros((64, HDIM), F32))
        for s in range(8):
            pc[way, s] = (base + ea[way, s]).astype(BF16)
        rc[way, rows_of(me, 64), :] = pc[way, me]
        for i in range(1, 8):
            c_copy(way, i, me).start()

    def exchange_end(way):
        for i in range(1, 8):
            c_copy(way, i, lax.rem(me - i + 8, 8)).wait()

    exchange_a(0, st[nblocks])

    loads[2].wait()

    def causal(scores):
        row = lax.broadcasted_iota(jnp.int32, (BLOCK, BLOCK), 0)
        col = lax.broadcasted_iota(jnp.int32, (BLOCK, BLOCK), 1)
        return jnp.where(col <= row, scores, jnp.zeros_like(scores)).astype(BF16)

    def score_step(b, carry):
        rows = rows_of(b, BLOCK)
        for h in range(heads):
            cols = slice(h * HDIM, (h + 1) * HDIM)
            sc[b, h] = causal(dot_nt(q[rows, cols], k[rows, cols]))
        return carry

    lax.fori_loop(0, 8, score_step, 0)
    exchange_b(0)
    lax.fori_loop(8, 16, score_step, 0)
    exchange_c(0)

    w_load(3).wait()

    def gn_own(half, carry):
        gn[rows_of(hi * 2 + half, 256), :] = dot_nt(
            d[rows_of(half, 256), :], w[rows_of(hi, 512), :]
        ).astype(BF16)
        return carry

    lax.fori_loop(0, 2, gn_own, 0)
    exchange_end(0)

    def nm_copy(j, r):
        target = lax.rem(hi + offset(j), 4)
        return pltpu.make_async_remote_copy(
            src_ref=nm.at[rows_of(target * 4 + r, BLOCK), :],
            dst_ref=nr.at[rows_of(r, BLOCK), rows_of(hi, 512)],
            send_sem=nm_ssem.at[j, r],
            recv_sem=nm_rsem.at[j, r],
            device_id=across(offset(j)),
            device_id_type=MESH,
        )

    def nm_arrival(j, r):
        source = lax.rem(hi - offset(j) + 4, 4)
        return pltpu.make_async_remote_copy(
            src_ref=nm.at[rows_of(source * 4 + r, BLOCK), :],
            dst_ref=nr.at[rows_of(r, BLOCK), rows_of(source, 512)],
            send_sem=nm_ssem.at[j, r],
            recv_sem=nm_rsem.at[j, r],
            device_id=across(offset(j)),
            device_id_type=MESH,
        )

    def forward_step(i, carry):
        own = i // 12
        j = lax.rem(i, 3)
        r = (1 - own) * (i // 3) + own * (i - 12)
        b = lax.rem(hi + (1 - own) * offset(j), 4) * 4 + r
        rows = rows_of(b, BLOCK)
        for h in range(heads):
            cols = slice(h * HDIM, (h + 1) * HDIM)
            before = (rc[0, h * HDIM:(h + 1) * HDIM, :].astype(F32) + st[b, h]).astype(BF16)
            pb[b, h] = before
            attended = dot_nn(
                jnp.concatenate([sc[b, h], q[rows, cols]], axis=1),
                jnp.concatenate([v[rows, cols], before], axis=0),
            )
            inverse = lax.rsqrt(
                jnp.mean(attended * attended, axis=-1, keepdims=True) + EPSILON
            )
            scaled = attended * inverse
            unit[rows, cols] = scaled
            inv[rows, cols] = jnp.broadcast_to(inverse, (BLOCK, HDIM))
            nm[rows, cols] = (scaled * gain[:, cols].astype(F32)).astype(BF16)

        @pl.when(own == 0)
        def _():
            nm_copy(j, r).start()

        @pl.when(own == 1)
        def _():
            nr[rows_of(r, BLOCK), rows_of(hi, 512)] = nm[rows, :]

        return carry

    lax.fori_loop(0, nblocks, forward_step, 0)

    def gq_copy(b):
        rows = rows_of(b, BLOCK)
        return pltpu.make_async_copy(sq.at[rows, :], grad_query.at[rows, :], gq_sem.at[b])

    def gk_copy(b):
        rows = rows_of(b, BLOCK)
        return pltpu.make_async_copy(sk.at[rows, :], grad_key.at[rows, :], gk_sem.at[b])

    def gv_copy(b):
        rows = rows_of(b, BLOCK)
        return pltpu.make_async_copy(sv.at[rows, :], grad_value.at[rows, :], gv_sem.at[b])

    def backward_block(b):
        rows = rows_of(b, BLOCK)
        for h in range(heads):
            cols = slice(h * HDIM, (h + 1) * HDIM)
            grad_unit = gn[rows, cols].astype(F32) * gain[:, cols].astype(F32)
            scaled = unit[rows, cols]
            inner = jnp.mean(grad_unit * scaled, axis=-1, keepdims=True)
            grad = (inv[rows, cols] * (grad_unit - scaled * inner)).astype(BF16)
            g[rows, cols] = grad
            both = dot_nt(grad, jnp.concatenate([v[rows, cols], pb[b, h]], axis=0))
            weights = causal(both[:, :BLOCK])
            gsc[b, h] = weights
            bg[b, h] = dot_tn(q[rows, cols], grad)
            sq[rows, cols] = (dot_nn(weights, k[rows, cols]) + both[:, BLOCK:]).astype(BF16)
        gq_copy(b).start()

    def backward_step(i, carry):
        far_away = (i + 12) // 16
        t = jnp.maximum(i - 4, 0)
        j = lax.rem(t, 3)
        r = far_away * (t // 3) + (1 - far_away) * i

        @pl.when((far_away == 1) & (lax.rem(r, 2) == 0))
        def _():
            gn_arrival(j, r // 2).wait_recv()

        backward_block(lax.rem(hi - far_away * offset(j) + 4, 4) * 4 + r)
        return carry

    lax.fori_loop(0, nblocks, backward_step, 0)

    def suffix_step(i, total):
        b = nblocks - 1 - i
        fresh = bg[b]
        bg[b] = total
        return total + fresh

    def suffix_head(h):
        def step(i, total):
            b = nblocks - 1 - i
            fresh = bg[b, h]
            bg[b, h] = total
            return total + fresh

        return lax.fori_loop(0, nblocks, step, jnp.zeros((HDIM, HDIM), F32))

    for h in range(heads):
        st[0, h] = suffix_head(h)
    exchange_a(1, st[0])
    exchange_b(1)
    exchange_c(1)
    exchange_end(1)

    def final_step(b, carry):
        rows = rows_of(b, BLOCK)
        for h in range(heads):
            cols = slice(h * HDIM, (h + 1) * HDIM)
            after = (rc[1, h * HDIM:(h + 1) * HDIM, :].astype(F32) + bg[b, h]).astype(BF16)
            sk[rows, cols] = (
                dot_tn(gsc[b, h], q[rows, cols]) + dot_nt(v[rows, cols], after)
            ).astype(BF16)
            sv[rows, cols] = (
                dot_tn(sc[b, h], g[rows, cols]) + dot_nn(k[rows, cols], after)
            ).astype(BF16)
        gk_copy(b).start()
        gv_copy(b).start()
        return carry

    lax.fori_loop(0, nblocks, final_step, 0)

    def out_copy(r):
        rows = rows_of(r, BLOCK)
        return pltpu.make_async_copy(so.at[rows, :], out.at[rows, :], out_sem.at[r])

    def out_step(r, carry):
        for j in range(3):
            nm_arrival(j, r).wait_recv()
        rows = rows_of(r, BLOCK)

        def out_columns(n, inner):
            so[rows, rows_of(n, 512)] = dot_nn(nr[rows, :], w[:, rows_of(n, 512)]).astype(BF16)
            return inner

        lax.fori_loop(0, 4, out_columns, 0)
        out_copy(r).start()
        return carry

    lax.fori_loop(0, 4, out_step, 0)

    def drain(i, carry):
        j, r = i // 4, lax.rem(i, 4)
        nm_copy(j, r).wait_send()

        @pl.when(r < 2)
        def _():
            gn_copy(j, r).wait_send()

        return carry

    lax.fori_loop(0, 12, drain, 0)

    def drain_blocks(b, carry):
        gq_copy(b).wait()
        gk_copy(b).wait()
        gv_copy(b).wait()
        return carry

    lax.fori_loop(0, nblocks, drain_blocks, 0)
    for r in range(4):
        out_copy(r).wait()


def on_device(query, key, value, gain, w_out, d_out):
    tokens, width = query.shape
    hbm = pl.BlockSpec(memory_space=pl.ANY)
    vmem = pl.BlockSpec(memory_space=pltpu.VMEM)
    heads, nblocks = 4, 16
    tall = (tokens, width)
    squares = (nblocks, heads, HDIM, HDIM)
    dma = pltpu.SemaphoreType.DMA
    return pl.pallas_call(
        kernel,
        out_shape=(
            jax.ShapeDtypeStruct(d_out.shape, BF16),
            jax.ShapeDtypeStruct(tall, BF16),
            jax.ShapeDtypeStruct(tall, BF16),
            jax.ShapeDtypeStruct(tall, BF16),
        ),
        in_specs=[hbm, hbm, hbm, vmem, hbm, hbm],
        out_specs=(hbm, hbm, hbm, hbm),
        scratch_shapes=[
            pltpu.VMEM(tall, BF16),
            pltpu.VMEM(tall, BF16),
            pltpu.VMEM(tall, BF16),
            pltpu.VMEM(w_out.shape, BF16),
            pltpu.VMEM(d_out.shape, BF16),
            pltpu.VMEM((3, 512, width), BF16),
            pltpu.VMEM(tall, BF16),
            pltpu.VMEM(tall, BF16),
            pltpu.VMEM(d_out.shape, BF16),
            pltpu.VMEM(squares, BF16),
            pltpu.VMEM(squares, BF16),
            pltpu.VMEM(tall, BF16),
            pltpu.VMEM(squares, BF16),
            pltpu.VMEM((nblocks + 1, heads, HDIM, HDIM), F32),
            pltpu.VMEM(squares, F32),
            pltpu.VMEM(tall, F32),
            pltpu.VMEM(tall, F32),
            pltpu.VMEM(tall, BF16),
            pltpu.VMEM(tall, BF16),
            pltpu.VMEM(tall, BF16),
            pltpu.VMEM(d_out.shape, BF16),
            pltpu.VMEM((2, 512, HDIM), BF16),
            pltpu.VMEM((2, 8, 64, HDIM), BF16),
            pltpu.VMEM((2, 8, 64, HDIM), F32),
            pltpu.VMEM((2, 64, HDIM), F32),
            pltpu.VMEM((2, 4, 64, HDIM), F32),
            pltpu.VMEM((2, 8, 64, HDIM), BF16),
            pltpu.VMEM((2, 512, HDIM), BF16),
            dma((4,)), dma((4,)), dma((3, 2)), dma((3, 2)), dma((3, 4)), dma((3, 4)),
            dma((2, 7)), dma((2, 7)), dma((2, 3)), dma((2, 3)), dma((2, 7)), dma((2, 7)),
            dma((16,)), dma((16,)), dma((16,)), dma((4,)),
        ],
        compiler_params=pltpu.CompilerParams(
            collective_id=0, has_side_effects=True, vmem_limit_bytes=62 * 2**20
        ),
    )(query, key, value, gain.reshape(1, width), w_out, d_out)


def solution(mesh):
    in_specs = (
        P("ctx", "head"), P("ctx", "head"), P("ctx", "head"), P("head"), P(),
        P(("ctx", "head"), None),
    )
    out_specs = (
        P(("ctx", "head"), None), P("ctx", "head"), P("ctx", "head"), P("ctx", "head"),
    )
    return jax.shard_map(
        on_device, mesh=mesh, in_specs=in_specs, out_specs=out_specs, check_vma=False
    )
```

```python
import jax
import jax.numpy as jnp
from jax import lax
from jax.experimental import pallas as pl
from jax.experimental.pallas import tpu as pltpu
from jax.sharding import PartitionSpec as P

HDIM = 128
BLOCK = 128
EPSILON = 1e-06
MESH = pl.DeviceIdType.MESH
F32 = jnp.float32
BF16 = jnp.bfloat16


def rows_of(index, size):
    return pl.ds(pl.multiple_of(index * size, size), size)


def dot_nn(a, b):
    return jnp.dot(a, b, preferred_element_type=F32)


def dot_nt(a, b):
    return lax.dot_general(a, b, (((1,), (1,)), ((), ())), preferred_element_type=F32)


def dot_tn(a, b):
    return lax.dot_general(a, b, (((0,), (0,)), ((), ())), preferred_element_type=F32)


def kernel(
    query, key, value, gain, w_out, d_out,
    so, sq, sk, sv,
    q, k, v, w, d, gn_send, gn, nm, nr, sc, gsc, g, pb, st, bg, unit, inv, run, acc,
    tb, ra, ea, rs, rb, pc, rc,
    load_sem, w_sem, gn_ssem, gn_rsem, nm_ssem, nm_rsem,
    a_ssem, a_rsem, b_ssem, b_rsem, c_ssem, c_rsem,
):
    ci = lax.axis_index("ctx")
    hi = lax.axis_index("head")
    y = ci // 8
    me = lax.rem(ci, 8)
    heads = 4
    nblocks = 16

    def w_load(i):
        h = lax.rem(hi + (1 + 2 * i - 3 * (i // 2)) * (1 - i // 3), 4)
        return pltpu.make_async_copy(
            w_out.at[rows_of(h, 512), :], w.at[rows_of(h, 512), :], w_sem.at[i]
        )

    loads = (
        pltpu.make_async_copy(key, k, load_sem.at[1]),
        pltpu.make_async_copy(value, v, load_sem.at[2]),
        pltpu.make_async_copy(query, q, load_sem.at[3]),
    )
    pltpu.make_async_copy(d_out, d, load_sem.at[0]).start()
    w_load(0).start()
    w_load(1).start()
    loads[0].start()
    loads[1].start()
    w_load(2).start()
    loads[2].start()
    w_load(3).start()
    scales = gain[...].astype(F32).reshape(1, 512)

    def near(i):
        return {"ctx": y * 8 + lax.rem(me + i, 8)}

    def far(i):
        return {"ctx": lax.rem(y + i, 4) * 8 + me}

    def across(o):
        return {"head": lax.rem(hi + o, 4)}

    barrier = pltpu.get_barrier_semaphore()
    for peer in (
        [across(o) for o in (1, 2, 3)]
        + [near(i) for i in range(1, 8)]
        + [far(i) for i in range(1, 4)]
    ):
        pl.semaphore_signal(barrier, inc=1, device_id=peer, device_id_type=MESH)
    pl.semaphore_wait(barrier, 13)

    def offset(j):
        return 1 + 2 * j - 3 * (j // 2)

    def gn_copy(j, half):
        return pltpu.make_async_remote_copy(
            src_ref=gn_send.at[j, rows_of(half, 256), :],
            dst_ref=gn.at[rows_of(hi * 2 + half, 256), :],
            send_sem=gn_ssem.at[j, half],
            recv_sem=gn_rsem.at[j, half],
            device_id=across(offset(j)),
            device_id_type=MESH,
        )

    def gn_arrival(j, half):
        source = lax.rem(hi - offset(j) + 4, 4)
        return pltpu.make_async_remote_copy(
            src_ref=gn_send.at[j, rows_of(half, 256), :],
            dst_ref=gn.at[rows_of(source * 2 + half, 256), :],
            send_sem=gn_ssem.at[j, half],
            recv_sem=gn_rsem.at[j, half],
            device_id=across(offset(j)),
            device_id_type=MESH,
        )

    pltpu.make_async_copy(d_out, d, load_sem.at[0]).wait()

    def gn_step(i, carry):
        half, j = i // 3, lax.rem(i, 3)

        @pl.when(half == 0)
        def _():
            w_load(j).wait()

        h = lax.rem(hi + offset(j), 4)
        gn_send[j, rows_of(half, 256), :] = dot_nt(
            d[rows_of(half, 256), :], w[rows_of(h, 512), :]
        ).astype(BF16)
        gn_copy(j, half).start()
        return carry

    lax.fori_loop(0, 3, gn_step, 0)

    loads[0].wait()
    loads[1].wait()
    run[...] = jnp.zeros((2, heads, HDIM, HDIM), F32)

    def state_step(i, carry):
        for h in range(heads):
            cols = slice(h * HDIM, (h + 1) * HDIM)
            total = run[0, h]
            for u in range(4):
                b = i * 4 + u
                rows = rows_of(b, BLOCK)
                st[b, h] = total
                total = total + dot_tn(k[rows, cols], v[rows, cols])
            run[0, h] = total
        return carry

    lax.fori_loop(0, 4, state_step, 0)

    def a_copy(way, i, slot):
        return pltpu.make_async_remote_copy(
            src_ref=tb.at[way, rows_of(lax.rem(me + i, 8), 64), :],
            dst_ref=ra.at[way, slot],
            send_sem=a_ssem.at[way, i - 1],
            recv_sem=a_rsem.at[way, i - 1],
            device_id=near(i),
            device_id_type=MESH,
        )

    def b_copy(way, i, slot):
        return pltpu.make_async_remote_copy(
            src_ref=rs.at[way],
            dst_ref=rb.at[way, slot],
            send_sem=b_ssem.at[way, i - 1],
            recv_sem=b_rsem.at[way, i - 1],
            device_id=far(i),
            device_id_type=MESH,
        )

    def c_copy(way, i, slot):
        return pltpu.make_async_remote_copy(
            src_ref=pc.at[way, lax.rem(me + i, 8)],
            dst_ref=rc.at[way, rows_of(slot, 64), :],
            send_sem=c_ssem.at[way, i - 1],
            recv_sem=c_rsem.at[way, i - 1],
            device_id=near(i),
            device_id_type=MESH,
        )

    def exchange_a(way, total):
        tb[way] = total.reshape(heads * HDIM, HDIM).astype(BF16)
        ra[way, me] = tb[way, rows_of(me, 64), :]
        for i in range(1, 8):
            a_copy(way, i, me).start()

    def exchange_b(way):
        for i in range(1, 8):
            a_copy(way, i, lax.rem(me - i + 8, 8)).wait()
        run = jnp.zeros((64, HDIM), F32)
        for s in reversed(range(8)) if way else range(8):
            ea[way, s] = run
            run = run + ra[way, s].astype(F32)
        rs[way] = run
        rb[way, y] = jnp.zeros((64, HDIM), F32)
        for i in range(1, 4):
            b_copy(way, i, y).start()

    def exchange_c(way):
        for i in range(1, 4):
            b_copy(way, i, lax.rem(y - i + 4, 4)).wait()
        base = jnp.zeros((64, HDIM), F32)
        for s in range(4):
            passed = s > y if way else s < y
            base = base + jnp.where(passed, rb[way, s], jnp.zeros((64, HDIM), F32))
        for s in range(8):
            pc[way, s] = (base + ea[way, s]).astype(BF16)
        rc[way, rows_of(me, 64), :] = pc[way, me]
        for i in range(1, 8):
            c_copy(way, i, me).start()

    def exchange_end(way):
        for i in range(1, 8):
            c_copy(way, i, lax.rem(me - i + 8, 8)).wait()

    exchange_a(0, run[0])
    lax.fori_loop(3, 6, gn_step, 0)
    exchange_b(0)
    loads[2].wait()

    def causal(scores):
        row = lax.broadcasted_iota(jnp.int32, (BLOCK, BLOCK), 0)
        col = lax.broadcasted_iota(jnp.int32, (BLOCK, BLOCK), 1)
        return jnp.where(col <= row, scores, jnp.zeros_like(scores)).astype(BF16)

    def score_step(i, carry):
        for u in range(4):
            b = i * 4 + u
            rows = rows_of(b, BLOCK)
            for h in range(heads):
                cols = slice(h * HDIM, (h + 1) * HDIM)
                sc[b, h] = causal(dot_nt(q[rows, cols], k[rows, cols]))
        return carry

    lax.fori_loop(0, 4, score_step, 0)
    exchange_c(0)

    w_load(3).wait()

    def gn_own(half, carry):
        gn[rows_of(hi * 2 + half, 256), :] = dot_nt(
            d[rows_of(half, 256), :], w[rows_of(hi, 512), :]
        ).astype(BF16)
        return carry

    lax.fori_loop(0, 2, gn_own, 0)
    exchange_end(0)

    def nm_copy(j, half):
        target = lax.rem(hi + offset(j), 4)
        return pltpu.make_async_remote_copy(
            src_ref=nm.at[rows_of(target * 2 + half, 256), :],
            dst_ref=nr.at[rows_of(half, 256), rows_of(hi, 512)],
            send_sem=nm_ssem.at[j, half],
            recv_sem=nm_rsem.at[j, half],
            device_id=across(offset(j)),
            device_id_type=MESH,
        )

    def nm_arrival(j, half):
        source = lax.rem(hi - offset(j) + 4, 4)
        return pltpu.make_async_remote_copy(
            src_ref=nm.at[rows_of(source * 2 + half, 256), :],
            dst_ref=nr.at[rows_of(half, 256), rows_of(source, 512)],
            send_sem=nm_ssem.at[j, half],
            recv_sem=nm_rsem.at[j, half],
            device_id=across(offset(j)),
            device_id_type=MESH,
        )

    def forward_block(b):
        rows = rows_of(b, BLOCK)
        for h in range(heads):
            cols = slice(h * HDIM, (h + 1) * HDIM)
            before = (rc[0, h * HDIM:(h + 1) * HDIM, :].astype(F32) + st[b, h]).astype(BF16)
            pb[b, h] = before
            attended = dot_nn(
                jnp.concatenate([sc[b, h], q[rows, cols]], axis=1),
                jnp.concatenate([v[rows, cols], before], axis=0),
            )
            inverse = lax.rsqrt(
                jnp.mean(attended * attended, axis=-1, keepdims=True) + EPSILON
            )
            scaled = attended * inverse
            unit[rows, cols] = scaled
            inv[rows, cols] = jnp.broadcast_to(inverse, (BLOCK, HDIM))
            nm[rows, cols] = (scaled * scales[:, cols]).astype(BF16)

    def forward_step(i, carry):
        own = i // 6
        j = lax.rem(i, 3)
        half = (1 - own) * (i // 3) + own * (i - 6)
        pair = lax.rem(hi + (1 - own) * offset(j), 4) * 2 + half
        for u in range(2):
            forward_block(pair * 2 + u)

        @pl.when(own == 0)
        def _():
            nm_copy(j, half).start()

        @pl.when(own == 1)
        def _():
            nr[rows_of(half, 256), rows_of(hi, 512)] = nm[rows_of(pair, 256), :]

        return carry

    lax.fori_loop(0, 8, forward_step, 0)

    def backward_block(b):
        rows = rows_of(b, BLOCK)
        for h in range(heads):
            cols = slice(h * HDIM, (h + 1) * HDIM)
            grad_unit = gn[rows, cols].astype(F32) * scales[:, cols]
            scaled = unit[rows, cols]
            inner = jnp.mean(grad_unit * scaled, axis=-1, keepdims=True)
            grad = (inv[rows, cols] * (grad_unit - scaled * inner)).astype(BF16)
            g[rows, cols] = grad
            both = dot_nt(grad, jnp.concatenate([v[rows, cols], pb[b, h]], axis=0))
            weights = causal(both[:, :BLOCK])
            gsc[b, h] = weights
            fresh = dot_tn(q[rows, cols], grad)
            bg[b, h] = fresh
            run[1, h] = run[1, h] + fresh
            sq[rows, cols] = (dot_nn(weights, k[rows, cols]) + both[:, BLOCK:]).astype(BF16)

    def backward_step(i, carry):
        far_away = (i + 6) // 8
        t = jnp.maximum(i - 2, 0)
        j = lax.rem(t, 3)
        half = far_away * (t // 3) + (1 - far_away) * i

        @pl.when(far_away == 1)
        def _():
            gn_arrival(j, half).wait_recv()

        pair = lax.rem(hi - far_away * offset(j) + 4, 4) * 2 + half
        for u in range(2):
            backward_block(pair * 2 + u)
        return carry

    lax.fori_loop(0, 8, backward_step, 0)
    exchange_a(1, run[1])

    def suffix_head(h):
        def step(i, total):
            b = nblocks - 1 - i
            fresh = bg[b, h]
            bg[b, h] = total
            return total + fresh

        return lax.fori_loop(0, nblocks, step, jnp.zeros((HDIM, HDIM), F32))

    for h in range(heads):
        suffix_head(h)
    exchange_b(1)
    exchange_c(1)

    for j in range(3):
        nm_arrival(j, 0).wait_recv()

    def out_columns(n, carry):
        so[:256, rows_of(n, 512)] = dot_nn(nr[:256, :], w[:, rows_of(n, 512)]).astype(BF16)
        return carry

    lax.fori_loop(0, 4, out_columns, 0)
    exchange_end(1)

    def final_block(b):
        rows = rows_of(b, BLOCK)
        for h in range(heads):
            cols = slice(h * HDIM, (h + 1) * HDIM)
            after = (rc[1, h * HDIM:(h + 1) * HDIM, :].astype(F32) + bg[b, h]).astype(BF16)
            sk[rows, cols] = (
                dot_tn(gsc[b, h], q[rows, cols]) + dot_nt(v[rows, cols], after)
            ).astype(BF16)
            sv[rows, cols] = (
                dot_tn(sc[b, h], g[rows, cols]) + dot_nn(k[rows, cols], after)
            ).astype(BF16)

    def final_step(i, carry):
        for u in range(2):
            final_block(i * 2 + u)
        return carry

    lax.fori_loop(0, 8, final_step, 0)

    def late_part(source, n):
        return dot_nn(
            nr[256:, rows_of(source, 512)], w[rows_of(source, 512), rows_of(n, 512)]
        )

    def late_own(n, carry):
        acc[:, rows_of(n, 512)] = late_part(hi, n)
        return carry

    lax.fori_loop(0, 4, late_own, 0)
    for j in range(2):
        nm_arrival(j, 1).wait_recv()

        def late_add(n, carry):
            source = lax.rem(hi - offset(j) + 4, 4)
            cols = rows_of(n, 512)
            acc[:, cols] = acc[:, cols] + late_part(source, n)
            return carry

        lax.fori_loop(0, 4, late_add, 0)
    nm_arrival(2, 1).wait_recv()

    def late_last(n, carry):
        cols = rows_of(n, 512)
        so[256:, cols] = (acc[:, cols] + late_part(lax.rem(hi + 2, 4), n)).astype(BF16)
        return carry

    lax.fori_loop(0, 4, late_last, 0)
    for j in range(3):
        for half in range(2):
            gn_copy(j, half).wait_send()
            nm_copy(j, half).wait_send()


def store_kernel(a, b, c, d, a_out, b_out, c_out, d_out, sem):
    copies = [
        pltpu.make_async_copy(held, placed, sem.at[i])
        for i, (held, placed) in enumerate(((a, a_out), (b, b_out), (c, c_out), (d, d_out)))
    ]
    for copy in copies:
        copy.start()
    for copy in copies:
        copy.wait()


def on_device(query, key, value, gain, w_out, d_out):
    tokens, width = query.shape
    hbm = pl.BlockSpec(memory_space=pl.ANY)
    vmem = pl.BlockSpec(memory_space=pltpu.VMEM)
    heads, nblocks = 4, 16
    tall = (tokens, width)
    squares = (nblocks, heads, HDIM, HDIM)
    dma = pltpu.SemaphoreType.DMA
    held = pl.pallas_call(
        kernel,
        out_shape=(
            pltpu.VMEM(d_out.shape, BF16),
            pltpu.VMEM(tall, BF16),
            pltpu.VMEM(tall, BF16),
            pltpu.VMEM(tall, BF16),
        ),
        in_specs=[hbm, hbm, hbm, vmem, hbm, hbm],
        out_specs=(vmem, vmem, vmem, vmem),
        scratch_shapes=[
            pltpu.VMEM(tall, BF16),
            pltpu.VMEM(tall, BF16),
            pltpu.VMEM(tall, BF16),
            pltpu.VMEM(w_out.shape, BF16),
            pltpu.VMEM(d_out.shape, BF16),
            pltpu.VMEM((3, 512, width), BF16),
            pltpu.VMEM(tall, BF16),
            pltpu.VMEM(tall, BF16),
            pltpu.VMEM(d_out.shape, BF16),
            pltpu.VMEM(squares, BF16),
            pltpu.VMEM(squares, BF16),
            pltpu.VMEM(tall, BF16),
            pltpu.VMEM(squares, BF16),
            pltpu.VMEM(squares, F32),
            pltpu.VMEM(squares, F32),
            pltpu.VMEM(tall, F32),
            pltpu.VMEM(tall, F32),
            pltpu.VMEM((2, heads, HDIM, HDIM), F32),
            pltpu.VMEM((256, d_out.shape[1]), F32),
            pltpu.VMEM((2, 512, HDIM), BF16),
            pltpu.VMEM((2, 8, 64, HDIM), BF16),
            pltpu.VMEM((2, 8, 64, HDIM), F32),
            pltpu.VMEM((2, 64, HDIM), F32),
            pltpu.VMEM((2, 4, 64, HDIM), F32),
            pltpu.VMEM((2, 8, 64, HDIM), BF16),
            pltpu.VMEM((2, 512, HDIM), BF16),
            dma((4,)), dma((4,)), dma((3, 2)), dma((3, 2)), dma((3, 2)), dma((3, 2)),
            dma((2, 7)), dma((2, 7)), dma((2, 3)), dma((2, 3)), dma((2, 7)), dma((2, 7)),
        ],
        compiler_params=pltpu.CompilerParams(
            collective_id=0, has_side_effects=True, vmem_limit_bytes=54 * 2**20
        ),
    )(query, key, value, gain, w_out, d_out)
    return pl.pallas_call(
        store_kernel,
        out_shape=tuple(jax.ShapeDtypeStruct(x.shape, BF16) for x in held),
        in_specs=[vmem] * 4,
        out_specs=(hbm,) * 4,
        scratch_shapes=[dma((4,))],
        compiler_params=pltpu.CompilerParams(vmem_limit_bytes=2**20),
    )(*held)


def solution(mesh):
    in_specs = (
        P("ctx", "head"), P("ctx", "head"), P("ctx", "head"), P("head"), P(),
        P(("ctx", "head"), None),
    )
    out_specs = (
        P(("ctx", "head"), None), P("ctx", "head"), P("ctx", "head"), P("ctx", "head"),
    )
    return jax.shard_map(
        on_device, mesh=mesh, in_specs=in_specs, out_specs=out_specs, check_vma=False
    )
```

```python
import jax
import jax.numpy as jnp
from jax import lax
from jax.experimental import pallas as pl
from jax.experimental.pallas import tpu as pltpu
from jax.sharding import PartitionSpec as P

HDIM = 128
BLOCK = 128
EPSILON = 1e-06
MESH = pl.DeviceIdType.MESH
F32 = jnp.float32
BF16 = jnp.bfloat16


def rows_of(index, size):
    return pl.ds(pl.multiple_of(index * size, size), size)


def dot_nn(a, b):
    return jnp.dot(a, b, preferred_element_type=F32)


def dot_nt(a, b):
    return lax.dot_general(a, b, (((1,), (1,)), ((), ())), preferred_element_type=F32)


def dot_tn(a, b):
    return lax.dot_general(a, b, (((0,), (0,)), ((), ())), preferred_element_type=F32)


def kernel(
    query, key, value, gain, w_out, d_out,
    so, sq, sk, sv, acc, nl, wl,
    q, k, v, w, d, gn_send, gn, nm, nr, sc, gsc, g, pb, st, bg, unit, inv, run,
    tb, ra, ea, rs, rb, pc, rc,
    load_sem, w_sem, gn_ssem, gn_rsem, nm_ssem, nm_rsem,
    a_ssem, a_rsem, b_ssem, b_rsem, c_ssem, c_rsem,
):
    ci = lax.axis_index("ctx")
    hi = lax.axis_index("head")
    y = ci // 8
    me = lax.rem(ci, 8)
    heads = 4
    nblocks = 16

    def w_load(i):
        h = lax.rem(hi + (1 + 2 * i - 3 * (i // 2)) * (1 - i // 3), 4)
        return pltpu.make_async_copy(
            w_out.at[rows_of(h, 512), :], w.at[rows_of(h, 512), :], w_sem.at[i]
        )

    loads = (
        pltpu.make_async_copy(key, k, load_sem.at[1]),
        pltpu.make_async_copy(value, v, load_sem.at[2]),
        pltpu.make_async_copy(query, q, load_sem.at[3]),
    )
    d_loads = [
        pltpu.make_async_copy(
            d_out.at[rows_of(half, 256), :], d.at[rows_of(half, 256), :], load_sem.at[4 * half]
        )
        for half in range(2)
    ]
    wl_load = pltpu.make_async_copy(
        w_out.at[rows_of(lax.rem(hi + 2, 4), 512), :], wl, load_sem.at[5]
    )
    d_loads[0].start()
    w_load(0).start()
    scales = gain[...].astype(F32).reshape(1, 512)

    def near(i):
        return {"ctx": y * 8 + lax.rem(me + i, 8)}

    def far(i):
        return {"ctx": lax.rem(y + i, 4) * 8 + me}

    def across(o):
        return {"head": lax.rem(hi + o, 4)}

    barrier = pltpu.get_barrier_semaphore()
    for peer in (
        [across(o) for o in (1, 2, 3)]
        + [near(i) for i in range(1, 8)]
        + [far(i) for i in range(1, 4)]
    ):
        pl.semaphore_signal(barrier, inc=1, device_id=peer, device_id_type=MESH)
    pl.semaphore_wait(barrier, 13)

    def offset(j):
        return 1 + 2 * j - 3 * (j // 2)

    def gn_copy(j, half):
        return pltpu.make_async_remote_copy(
            src_ref=gn_send.at[j, rows_of(half, 256), :],
            dst_ref=gn.at[rows_of(hi * 2 + half, 256), :],
            send_sem=gn_ssem.at[j, half],
            recv_sem=gn_rsem.at[j, half],
            device_id=across(offset(j)),
            device_id_type=MESH,
        )

    def gn_arrival(j, half):
        source = lax.rem(hi - offset(j) + 4, 4)
        return pltpu.make_async_remote_copy(
            src_ref=gn_send.at[j, rows_of(half, 256), :],
            dst_ref=gn.at[rows_of(source * 2 + half, 256), :],
            send_sem=gn_ssem.at[j, half],
            recv_sem=gn_rsem.at[j, half],
            device_id=across(offset(j)),
            device_id_type=MESH,
        )

    d_loads[0].wait()

    def gn_step(i, carry):
        half, j = i // 3, lax.rem(i, 3)

        @pl.when(half == 0)
        def _():
            w_load(j).wait()

        @pl.when(i == 0)
        def _():
            w_load(1).start()
            w_load(2).start()
            for load in loads:
                load.start()
            d_loads[1].start()
            w_load(3).start()
            wl_load.start()

        h = lax.rem(hi + offset(j), 4)
        gn_send[j, rows_of(half, 256), :] = dot_nt(
            d[rows_of(half, 256), :], w[rows_of(h, 512), :]
        ).astype(BF16)
        gn_copy(j, half).start()
        return carry

    lax.fori_loop(0, 3, gn_step, 0)

    loads[0].wait()
    loads[1].wait()
    run[...] = jnp.zeros((2, heads, HDIM, HDIM), F32)

    def state_step(i, carry):
        for h in range(heads):
            cols = slice(h * HDIM, (h + 1) * HDIM)
            total = run[0, h]
            for u in range(4):
                b = i * 4 + u
                rows = rows_of(b, BLOCK)
                st[b, h] = total
                total = total + dot_tn(k[rows, cols], v[rows, cols])
            run[0, h] = total
        return carry

    lax.fori_loop(0, 4, state_step, 0)

    def a_copy(way, i, slot):
        return pltpu.make_async_remote_copy(
            src_ref=tb.at[way, rows_of(lax.rem(me + i, 8), 64), :],
            dst_ref=ra.at[way, slot],
            send_sem=a_ssem.at[way, i - 1],
            recv_sem=a_rsem.at[way, i - 1],
            device_id=near(i),
            device_id_type=MESH,
        )

    def b_copy(way, i, slot):
        return pltpu.make_async_remote_copy(
            src_ref=rs.at[way],
            dst_ref=rb.at[way, slot],
            send_sem=b_ssem.at[way, i - 1],
            recv_sem=b_rsem.at[way, i - 1],
            device_id=far(i),
            device_id_type=MESH,
        )

    def c_copy(way, i, slot):
        return pltpu.make_async_remote_copy(
            src_ref=pc.at[way, lax.rem(me + i, 8)],
            dst_ref=rc.at[way, rows_of(slot, 64), :],
            send_sem=c_ssem.at[way, i - 1],
            recv_sem=c_rsem.at[way, i - 1],
            device_id=near(i),
            device_id_type=MESH,
        )

    def exchange_a(way, total):
        tb[way] = total.reshape(heads * HDIM, HDIM).astype(BF16)
        ra[way, me] = tb[way, rows_of(me, 64), :]
        for i in range(1, 8):
            a_copy(way, i, me).start()

    def exchange_b(way):
        for i in range(1, 8):
            a_copy(way, i, lax.rem(me - i + 8, 8)).wait()
        run = jnp.zeros((64, HDIM), F32)
        for s in reversed(range(8)) if way else range(8):
            ea[way, s] = run
            run = run + ra[way, s].astype(F32)
        rs[way] = run.astype(BF16)
        rb[way, y] = jnp.zeros((64, HDIM), BF16)
        for i in range(1, 4):
            b_copy(way, i, y).start()

    def exchange_c(way):
        for i in range(1, 4):
            b_copy(way, i, lax.rem(y - i + 4, 4)).wait()
        base = jnp.zeros((64, HDIM), F32)
        for s in range(4):
            passed = s > y if way else s < y
            base = base + jnp.where(passed, rb[way, s].astype(F32), jnp.zeros((64, HDIM), F32))
        for s in range(8):
            pc[way, s] = (base + ea[way, s]).astype(BF16)
        rc[way, rows_of(me, 64), :] = pc[way, me]
        for i in range(1, 8):
            c_copy(way, i, me).start()

    def exchange_end(way):
        for i in range(1, 8):
            c_copy(way, i, lax.rem(me - i + 8, 8)).wait()

    exchange_a(0, run[0])
    d_loads[1].wait()
    lax.fori_loop(3, 6, gn_step, 0)
    exchange_b(0)
    loads[2].wait()

    def causal(scores):
        row = lax.broadcasted_iota(jnp.int32, (BLOCK, BLOCK), 0)
        col = lax.broadcasted_iota(jnp.int32, (BLOCK, BLOCK), 1)
        return jnp.where(col <= row, scores, jnp.zeros_like(scores)).astype(BF16)

    def score_step(i, carry):
        for u in range(4):
            b = i * 4 + u
            rows = rows_of(b, BLOCK)
            for h in range(heads):
                cols = slice(h * HDIM, (h + 1) * HDIM)
                sc[b, h] = causal(dot_nt(q[rows, cols], k[rows, cols]))
        return carry

    lax.fori_loop(0, 4, score_step, 0)
    exchange_c(0)

    w_load(3).wait()

    def gn_own(half, carry):
        gn[rows_of(hi * 2 + half, 256), :] = dot_nt(
            d[rows_of(half, 256), :], w[rows_of(hi, 512), :]
        ).astype(BF16)
        return carry

    lax.fori_loop(0, 2, gn_own, 0)
    exchange_end(0)

    def nm_copy(j, half):
        target = lax.rem(hi + offset(j), 4)
        return pltpu.make_async_remote_copy(
            src_ref=nm.at[rows_of(target * 2 + half, 256), :],
            dst_ref=nr.at[rows_of(half, 256), rows_of(hi, 512)],
            send_sem=nm_ssem.at[j, half],
            recv_sem=nm_rsem.at[j, half],
            device_id=across(offset(j)),
            device_id_type=MESH,
        )

    def nm_arrival(j, half):
        source = lax.rem(hi - offset(j) + 4, 4)
        return pltpu.make_async_remote_copy(
            src_ref=nm.at[rows_of(source * 2 + half, 256), :],
            dst_ref=nr.at[rows_of(half, 256), rows_of(source, 512)],
            send_sem=nm_ssem.at[j, half],
            recv_sem=nm_rsem.at[j, half],
            device_id=across(offset(j)),
            device_id_type=MESH,
        )

    def forward_block(b):
        rows = rows_of(b, BLOCK)
        for h in range(heads):
            cols = slice(h * HDIM, (h + 1) * HDIM)
            before = (rc[0, h * HDIM:(h + 1) * HDIM, :].astype(F32) + st[b, h]).astype(BF16)
            pb[b, h] = before
            attended = dot_nn(
                jnp.concatenate([sc[b, h], q[rows, cols]], axis=1),
                jnp.concatenate([v[rows, cols], before], axis=0),
            )
            inverse = lax.rsqrt(
                jnp.mean(attended * attended, axis=-1, keepdims=True) + EPSILON
            )
            scaled = attended * inverse
            unit[rows, cols] = scaled
            inv[rows, cols] = jnp.broadcast_to(inverse, (BLOCK, HDIM))
            nm[rows, cols] = (scaled * scales[:, cols]).astype(BF16)

    def forward_step(i, carry):
        own = i // 6
        j = lax.rem(i, 3)
        half = (1 - own) * (i // 3) + own * (i - 6)
        pair = lax.rem(hi + (1 - own) * offset(j), 4) * 2 + half
        for u in range(2):
            forward_block(pair * 2 + u)

        @pl.when(own == 0)
        def _():
            nm_copy(j, half).start()

        @pl.when(own == 1)
        def _():
            nr[rows_of(half, 256), rows_of(hi, 512)] = nm[rows_of(pair, 256), :]

        return carry

    lax.fori_loop(0, 8, forward_step, 0)

    def backward_block(b):
        rows = rows_of(b, BLOCK)
        for h in range(heads):
            cols = slice(h * HDIM, (h + 1) * HDIM)
            grad_unit = gn[rows, cols].astype(F32) * scales[:, cols]
            scaled = unit[rows, cols]
            inner = jnp.mean(grad_unit * scaled, axis=-1, keepdims=True)
            grad = (inv[rows, cols] * (grad_unit - scaled * inner)).astype(BF16)
            g[rows, cols] = grad
            both = dot_nt(grad, jnp.concatenate([v[rows, cols], pb[b, h]], axis=0))
            weights = causal(both[:, :BLOCK])
            gsc[b, h] = weights
            fresh = dot_tn(q[rows, cols], grad)
            bg[b, h] = fresh
            run[1, h] = run[1, h] + fresh
            sq[rows, cols] = (dot_nn(weights, k[rows, cols]) + both[:, BLOCK:]).astype(BF16)

    def backward_step(i, carry):
        far_away = (i + 6) // 8
        t = jnp.maximum(i - 2, 0)
        j = lax.rem(t, 3)
        half = far_away * (t // 3) + (1 - far_away) * i

        @pl.when(far_away == 1)
        def _():
            gn_arrival(j, half).wait_recv()

        pair = lax.rem(hi - far_away * offset(j) + 4, 4) * 2 + half
        for u in range(2):
            backward_block(pair * 2 + u)
        return carry

    lax.fori_loop(0, 8, backward_step, 0)
    exchange_a(1, run[1])

    def suffix_head(h):
        def step(i, total):
            b = nblocks - 1 - i
            fresh = bg[b, h]
            bg[b, h] = total
            return total + fresh

        return lax.fori_loop(0, nblocks, step, jnp.zeros((HDIM, HDIM), F32))

    for h in range(heads):
        suffix_head(h)
    exchange_b(1)
    exchange_c(1)

    for j in range(3):
        nm_arrival(j, 0).wait_recv()

    def out_columns(n, carry):
        so[:, rows_of(n, 512)] = dot_nn(nr[:256, :], w[:, rows_of(n, 512)]).astype(BF16)
        return carry

    lax.fori_loop(0, 4, out_columns, 0)
    exchange_end(1)

    def final_block(b):
        rows = rows_of(b, BLOCK)
        for h in range(heads):
            cols = slice(h * HDIM, (h + 1) * HDIM)
            after = (rc[1, h * HDIM:(h + 1) * HDIM, :].astype(F32) + bg[b, h]).astype(BF16)
            sk[rows, cols] = (
                dot_tn(gsc[b, h], q[rows, cols]) + dot_nt(v[rows, cols], after)
            ).astype(BF16)
            sv[rows, cols] = (
                dot_tn(sc[b, h], g[rows, cols]) + dot_nn(k[rows, cols], after)
            ).astype(BF16)

    def final_step(i, carry):
        for u in range(2):
            final_block(i * 2 + u)
        return carry

    lax.fori_loop(0, 8, final_step, 0)

    def late_part(source, n):
        return dot_nn(
            nr[256:, rows_of(source, 512)], w[rows_of(source, 512), rows_of(n, 512)]
        )

    for j in range(2):
        nm_arrival(j, 1).wait_recv()

    def late_most(n, carry):
        total = late_part(hi, n)
        for j in range(2):
            total = total + late_part(lax.rem(hi - offset(j) + 4, 4), n)
        acc[:, rows_of(n, 512)] = total
        return carry

    lax.fori_loop(0, 4, late_most, 0)
    wl_load.wait()
    nm_arrival(2, 1).wait_recv()
    nl[...] = nr[256:, rows_of(lax.rem(hi + 2, 4), 512)]
    for j in range(3):
        for half in range(2):
            gn_copy(j, half).wait_send()
            nm_copy(j, half).wait_send()


def store_kernel(so, sq, sk, sv, acc, nl, wl, out, grad_query, grad_key, grad_value, late, sem):
    copies = [
        pltpu.make_async_copy(held, placed, sem.at[i])
        for i, (held, placed) in enumerate(
            ((sq, grad_query), (sk, grad_key), (sv, grad_value), (so, out.at[pl.ds(0, 256), :]))
        )
    ]
    for copy in copies:
        copy.start()
    for n in range(4):
        cols = pl.ds(n * 512, 512)
        late[:, cols] = (acc[:, cols] + dot_nn(nl[...], wl[:, cols])).astype(BF16)
        copy = pltpu.make_async_copy(
            late.at[:, cols], out.at[pl.ds(256, 256), cols], sem.at[4 + n]
        )
        copy.start()
        copies.append(copy)
    for copy in copies:
        copy.wait()


def on_device(query, key, value, gain, w_out, d_out):
    tokens, width = query.shape
    hbm = pl.BlockSpec(memory_space=pl.ANY)
    vmem = pl.BlockSpec(memory_space=pltpu.VMEM)
    heads, nblocks = 4, 16
    tall = (tokens, width)
    squares = (nblocks, heads, HDIM, HDIM)
    dma = pltpu.SemaphoreType.DMA
    held = pl.pallas_call(
        kernel,
        out_shape=(
            pltpu.VMEM((256, d_out.shape[1]), BF16),
            pltpu.VMEM(tall, BF16),
            pltpu.VMEM(tall, BF16),
            pltpu.VMEM(tall, BF16),
            pltpu.VMEM((256, d_out.shape[1]), F32),
            pltpu.VMEM((256, width), BF16),
            pltpu.VMEM((width, d_out.shape[1]), BF16),
        ),
        in_specs=[hbm, hbm, hbm, vmem, hbm, hbm],
        out_specs=(vmem,) * 7,
        scratch_shapes=[
            pltpu.VMEM(tall, BF16),
            pltpu.VMEM(tall, BF16),
            pltpu.VMEM(tall, BF16),
            pltpu.VMEM(w_out.shape, BF16),
            pltpu.VMEM(d_out.shape, BF16),
            pltpu.VMEM((3, 512, width), BF16),
            pltpu.VMEM(tall, BF16),
            pltpu.VMEM(tall, BF16),
            pltpu.VMEM(d_out.shape, BF16),
            pltpu.VMEM(squares, BF16),
            pltpu.VMEM(squares, BF16),
            pltpu.VMEM(tall, BF16),
            pltpu.VMEM(squares, BF16),
            pltpu.VMEM(squares, F32),
            pltpu.VMEM(squares, F32),
            pltpu.VMEM(tall, F32),
            pltpu.VMEM(tall, F32),
            pltpu.VMEM((2, heads, HDIM, HDIM), F32),
            pltpu.VMEM((2, 512, HDIM), BF16),
            pltpu.VMEM((2, 8, 64, HDIM), BF16),
            pltpu.VMEM((2, 8, 64, HDIM), F32),
            pltpu.VMEM((2, 64, HDIM), BF16),
            pltpu.VMEM((2, 4, 64, HDIM), BF16),
            pltpu.VMEM((2, 8, 64, HDIM), BF16),
            pltpu.VMEM((2, 512, HDIM), BF16),
            dma((6,)), dma((4,)), dma((3, 2)), dma((3, 2)), dma((3, 2)), dma((3, 2)),
            dma((2, 7)), dma((2, 7)), dma((2, 3)), dma((2, 3)), dma((2, 7)), dma((2, 7)),
        ],
        compiler_params=pltpu.CompilerParams(
            collective_id=0, has_side_effects=True, vmem_limit_bytes=51 * 2**20
        ),
    )(query, key, value, gain, w_out, d_out)
    return pl.pallas_call(
        store_kernel,
        out_shape=tuple(
            jax.ShapeDtypeStruct(shape, BF16) for shape in (d_out.shape, tall, tall, tall)
        ),
        in_specs=[vmem] * 7,
        out_specs=(hbm,) * 4,
        scratch_shapes=[pltpu.VMEM((256, d_out.shape[1]), BF16), dma((8,))],
        compiler_params=pltpu.CompilerParams(vmem_limit_bytes=4 * 2**20),
    )(*held)


def solution(mesh):
    in_specs = (
        P("ctx", "head"), P("ctx", "head"), P("ctx", "head"), P("head"), P(),
        P(("ctx", "head"), None),
    )
    out_specs = (
        P(("ctx", "head"), None), P("ctx", "head"), P("ctx", "head"), P("ctx", "head"),
    )
    return jax.shard_map(
        on_device, mesh=mesh, in_specs=in_specs, out_specs=out_specs, check_vma=False
    )
```

```python
import jax
import jax.numpy as jnp
from jax import lax
from jax.experimental import pallas as pl
from jax.experimental.pallas import tpu as pltpu
from jax.sharding import PartitionSpec as P

HDIM = 128
BLOCK = 128
EPSILON = 1e-06
MESH = pl.DeviceIdType.MESH
F32 = jnp.float32
BF16 = jnp.bfloat16


def rows_of(index, size):
    return pl.ds(pl.multiple_of(index * size, size), size)


def dot_nn(a, b):
    return jnp.dot(a, b, preferred_element_type=F32)


def dot_nt(a, b):
    return lax.dot_general(a, b, (((1,), (1,)), ((), ())), preferred_element_type=F32)


def dot_tn(a, b):
    return lax.dot_general(a, b, (((0,), (0,)), ((), ())), preferred_element_type=F32)


def kernel(
    query, key, value, gain, w_out, d_out,
    so, sq, sk, sv, acc, nl, wl,
    q, k, v, w, d, gn_send, gn, nm, nr, sc, gsc, g, pb, st, bg, unit, inv, run,
    tb, ra, ea, rs, rb, pc, rc,
    load_sem, w_sem, gn_ssem, gn_rsem, nm_ssem, nm_rsem,
    a_ssem, a_rsem, b_ssem, b_rsem, c_ssem, c_rsem,
):
    ci = lax.axis_index("ctx")
    hi = lax.axis_index("head")
    y = ci // 8
    me = lax.rem(ci, 8)
    heads = 4
    nblocks = 16

    def w_load(i):
        h = lax.rem(hi + (1 + 2 * i - 3 * (i // 2)) * (1 - i // 3), 4)
        return pltpu.make_async_copy(
            w_out.at[rows_of(h, 512), :], w.at[rows_of(h, 512), :], w_sem.at[i]
        )

    loads = (
        pltpu.make_async_copy(key, k, load_sem.at[1]),
        pltpu.make_async_copy(value, v, load_sem.at[2]),
        pltpu.make_async_copy(query, q, load_sem.at[3]),
    )
    d_loads = [
        pltpu.make_async_copy(
            d_out.at[rows_of(half, 256), :], d.at[rows_of(half, 256), :], load_sem.at[4 * half]
        )
        for half in range(2)
    ]
    wl_load = pltpu.make_async_copy(
        w_out.at[rows_of(lax.rem(hi + 2, 4), 512), :], wl, load_sem.at[5]
    )
    d_loads[0].start()
    w_load(0).start()
    scales = gain[...].astype(F32).reshape(1, 512)

    def near(i):
        return {"ctx": y * 8 + lax.rem(me + i, 8)}

    def far(i):
        return {"ctx": lax.rem(y + i, 4) * 8 + me}

    def across(o):
        return {"head": lax.rem(hi + o, 4)}

    barrier = pltpu.get_barrier_semaphore()
    for peer in (
        [across(o) for o in (1, 2, 3)]
        + [near(i) for i in range(1, 8)]
        + [far(i) for i in range(1, 4)]
    ):
        pl.semaphore_signal(barrier, inc=1, device_id=peer, device_id_type=MESH)
    pl.semaphore_wait(barrier, 13)

    def offset(j):
        return 1 + 2 * j - 3 * (j // 2)

    def gn_copy(j, half):
        return pltpu.make_async_remote_copy(
            src_ref=gn_send.at[j, rows_of(half, 256), :],
            dst_ref=gn.at[rows_of(hi * 2 + half, 256), :],
            send_sem=gn_ssem.at[j, half],
            recv_sem=gn_rsem.at[j, half],
            device_id=across(offset(j)),
            device_id_type=MESH,
        )

    def gn_arrival(j, half):
        source = lax.rem(hi - offset(j) + 4, 4)
        return pltpu.make_async_remote_copy(
            src_ref=gn_send.at[j, rows_of(half, 256), :],
            dst_ref=gn.at[rows_of(source * 2 + half, 256), :],
            send_sem=gn_ssem.at[j, half],
            recv_sem=gn_rsem.at[j, half],
            device_id=across(offset(j)),
            device_id_type=MESH,
        )

    d_loads[0].wait()

    def gn_step(i, carry):
        half, j = i // 3, lax.rem(i, 3)

        @pl.when(half == 0)
        def _():
            w_load(j).wait()

        @pl.when(i == 0)
        def _():
            w_load(1).start()
            w_load(2).start()
            for load in loads:
                load.start()
            d_loads[1].start()
            w_load(3).start()
            wl_load.start()

        h = lax.rem(hi + offset(j), 4)
        gn_send[j, rows_of(half, 256), :] = dot_nt(
            d[rows_of(half, 256), :], w[rows_of(h, 512), :]
        ).astype(BF16)
        gn_copy(j, half).start()
        return carry

    lax.fori_loop(0, 3, gn_step, 0)

    loads[0].wait()
    loads[1].wait()
    run[...] = jnp.zeros((2, heads, HDIM, HDIM), F32)

    def state_step(i, carry):
        for h in range(heads):
            cols = slice(h * HDIM, (h + 1) * HDIM)
            total = run[0, h]
            for u in range(4):
                b = i * 4 + u
                rows = rows_of(b, BLOCK)
                st[b, h] = total
                total = total + dot_tn(k[rows, cols], v[rows, cols])
            run[0, h] = total
        return carry

    lax.fori_loop(0, 4, state_step, 0)

    def a_copy(way, i, slot):
        return pltpu.make_async_remote_copy(
            src_ref=tb.at[way, rows_of(lax.rem(me + i, 8), 64), :],
            dst_ref=ra.at[way, slot],
            send_sem=a_ssem.at[way, i - 1],
            recv_sem=a_rsem.at[way, i - 1],
            device_id=near(i),
            device_id_type=MESH,
        )

    def b_copy(way, i, slot):
        return pltpu.make_async_remote_copy(
            src_ref=rs.at[way],
            dst_ref=rb.at[way, slot],
            send_sem=b_ssem.at[way, i - 1],
            recv_sem=b_rsem.at[way, i - 1],
            device_id=far(i),
            device_id_type=MESH,
        )

    def c_copy(way, i, slot):
        return pltpu.make_async_remote_copy(
            src_ref=pc.at[way, lax.rem(me + i, 8)],
            dst_ref=rc.at[way, rows_of(slot, 64), :],
            send_sem=c_ssem.at[way, i - 1],
            recv_sem=c_rsem.at[way, i - 1],
            device_id=near(i),
            device_id_type=MESH,
        )

    def exchange_a(way, total):
        tb[way] = total.reshape(heads * HDIM, HDIM).astype(BF16)
        ra[way, me] = tb[way, rows_of(me, 64), :]
        for i in range(1, 8):
            a_copy(way, i, me).start()

    def exchange_b(way):
        for i in range(1, 8):
            a_copy(way, i, lax.rem(me - i + 8, 8)).wait()
        run = jnp.zeros((64, HDIM), F32)
        for s in reversed(range(8)) if way else range(8):
            ea[way, s] = run
            run = run + ra[way, s].astype(F32)
        rs[way] = run.astype(BF16)
        rb[way, y] = jnp.zeros((64, HDIM), BF16)
        for i in range(1, 4):
            b_copy(way, i, y).start()

    def exchange_c(way):
        for i in range(1, 4):
            b_copy(way, i, lax.rem(y - i + 4, 4)).wait()
        base = jnp.zeros((64, HDIM), F32)
        for s in range(4):
            passed = s > y if way else s < y
            base = base + jnp.where(passed, rb[way, s].astype(F32), jnp.zeros((64, HDIM), F32))
        for s in range(8):
            pc[way, s] = (base + ea[way, s]).astype(BF16)
        rc[way, rows_of(me, 64), :] = pc[way, me]
        for i in range(1, 8):
            c_copy(way, i, me).start()

    def exchange_end(way):
        for i in range(1, 8):
            c_copy(way, i, lax.rem(me - i + 8, 8)).wait()

    exchange_a(0, run[0])
    d_loads[1].wait()
    lax.fori_loop(3, 6, gn_step, 0)
    exchange_b(0)
    loads[2].wait()

    def causal(scores):
        row = lax.broadcasted_iota(jnp.int32, (BLOCK, BLOCK), 0)
        col = lax.broadcasted_iota(jnp.int32, (BLOCK, BLOCK), 1)
        return jnp.where(col <= row, scores, jnp.zeros_like(scores)).astype(BF16)

    def score_step(i, carry):
        for u in range(4):
            b = i * 4 + u
            rows = rows_of(b, BLOCK)
            for h in range(heads):
                cols = slice(h * HDIM, (h + 1) * HDIM)
                sc[b, h] = causal(dot_nt(q[rows, cols], k[rows, cols]))
        return carry

    lax.fori_loop(0, 4, score_step, 0)
    exchange_c(0)

    w_load(3).wait()

    def gn_own(half, carry):
        gn[rows_of(hi * 2 + half, 256), :] = dot_nt(
            d[rows_of(half, 256), :], w[rows_of(hi, 512), :]
        ).astype(BF16)
        return carry

    lax.fori_loop(0, 2, gn_own, 0)
    exchange_end(0)

    def nm_copy(j, half):
        target = lax.rem(hi + offset(j), 4)
        return pltpu.make_async_remote_copy(
            src_ref=nm.at[rows_of(target * 2 + half, 256), :],
            dst_ref=nr.at[rows_of(half, 256), rows_of(hi, 512)],
            send_sem=nm_ssem.at[j, half],
            recv_sem=nm_rsem.at[j, half],
            device_id=across(offset(j)),
            device_id_type=MESH,
        )

    def nm_arrival(j, half):
        source = lax.rem(hi - offset(j) + 4, 4)
        return pltpu.make_async_remote_copy(
            src_ref=nm.at[rows_of(source * 2 + half, 256), :],
            dst_ref=nr.at[rows_of(half, 256), rows_of(source, 512)],
            send_sem=nm_ssem.at[j, half],
            recv_sem=nm_rsem.at[j, half],
            device_id=across(offset(j)),
            device_id_type=MESH,
        )

    def forward_block(b):
        rows = rows_of(b, BLOCK)
        for h in range(heads):
            cols = slice(h * HDIM, (h + 1) * HDIM)
            before = (rc[0, h * HDIM:(h + 1) * HDIM, :].astype(F32) + st[b, h]).astype(BF16)
            pb[b, h] = before
            attended = dot_nn(
                jnp.concatenate([sc[b, h], q[rows, cols]], axis=1),
                jnp.concatenate([v[rows, cols], before], axis=0),
            )
            inverse = lax.rsqrt(
                jnp.mean(attended * attended, axis=-1, keepdims=True) + EPSILON
            )
            scaled = attended * inverse
            unit[rows, cols] = scaled
            inv[rows, cols] = jnp.broadcast_to(inverse, (BLOCK, HDIM))
            nm[rows, cols] = (scaled * scales[:, cols]).astype(BF16)

    def forward_step(i, carry):
        own = i // 6
        j = lax.rem(i, 3)
        half = (1 - own) * (i // 3) + own * (i - 6)
        pair = lax.rem(hi + (1 - own) * offset(j), 4) * 2 + half
        for u in range(2):
            forward_block(pair * 2 + u)

        @pl.when(own == 0)
        def _():
            nm_copy(j, half).start()

        @pl.when(own == 1)
        def _():
            nr[rows_of(half, 256), rows_of(hi, 512)] = nm[rows_of(pair, 256), :]

        return carry

    lax.fori_loop(0, 8, forward_step, 0)

    def backward_block(b):
        rows = rows_of(b, BLOCK)
        for h in range(heads):
            cols = slice(h * HDIM, (h + 1) * HDIM)
            grad_unit = gn[rows, cols].astype(F32) * scales[:, cols]
            scaled = unit[rows, cols]
            inner = jnp.mean(grad_unit * scaled, axis=-1, keepdims=True)
            grad = (inv[rows, cols] * (grad_unit - scaled * inner)).astype(BF16)
            g[rows, cols] = grad
            both = dot_nt(grad, jnp.concatenate([v[rows, cols], pb[b, h]], axis=0))
            weights = causal(both[:, :BLOCK])
            gsc[b, h] = weights
            fresh = dot_tn(q[rows, cols], grad)
            bg[b, h] = fresh
            run[1, h] = run[1, h] + fresh
            sq[rows, cols] = (dot_nn(weights, k[rows, cols]) + both[:, BLOCK:]).astype(BF16)

    def backward_step(i, carry):
        far_away = (i + 6) // 8
        t = jnp.maximum(i - 2, 0)
        j = lax.rem(t, 3)
        half = far_away * (t // 3) + (1 - far_away) * i

        @pl.when(far_away == 1)
        def _():
            gn_arrival(j, half).wait_recv()

        pair = lax.rem(hi - far_away * offset(j) + 4, 4) * 2 + half
        for u in range(2):
            backward_block(pair * 2 + u)
        return carry

    lax.fori_loop(0, 8, backward_step, 0)
    exchange_a(1, run[1])

    def suffix_head(h):
        def step(i, total):
            b = nblocks - 1 - i
            fresh = bg[b, h]
            bg[b, h] = total
            return total + fresh

        return lax.fori_loop(0, nblocks, step, jnp.zeros((HDIM, HDIM), F32))

    for h in range(heads):
        suffix_head(h)
    exchange_b(1)
    exchange_c(1)

    for j in range(3):
        nm_arrival(j, 0).wait_recv()

    def out_columns(n, carry):
        so[:, rows_of(n, 512)] = dot_nn(nr[:256, :], w[:, rows_of(n, 512)]).astype(BF16)
        return carry

    lax.fori_loop(0, 4, out_columns, 0)
    exchange_end(1)

    def final_block(b):
        rows = rows_of(b, BLOCK)
        for h in range(heads):
            cols = slice(h * HDIM, (h + 1) * HDIM)
            after = (rc[1, h * HDIM:(h + 1) * HDIM, :].astype(F32) + bg[b, h]).astype(BF16)
            sk[rows, cols] = (
                dot_tn(gsc[b, h], q[rows, cols]) + dot_nt(v[rows, cols], after)
            ).astype(BF16)
            sv[rows, cols] = (
                dot_tn(sc[b, h], g[rows, cols]) + dot_nn(k[rows, cols], after)
            ).astype(BF16)

    def final_step(i, carry):
        for u in range(4):
            final_block(i * 4 + u)
        return carry

    lax.fori_loop(0, 4, final_step, 0)

    def late_part(source, n):
        return dot_nn(
            nr[256:, rows_of(source, 512)], w[rows_of(source, 512), rows_of(n, 512)]
        )

    for j in range(2):
        nm_arrival(j, 1).wait_recv()

    def late_most(n, carry):
        total = late_part(hi, n)
        for j in range(2):
            total = total + late_part(lax.rem(hi - offset(j) + 4, 4), n)
        acc[:, rows_of(n, 512)] = total
        return carry

    lax.fori_loop(0, 4, late_most, 0)
    wl_load.wait()
    nm_arrival(2, 1).wait_recv()
    nl[...] = nr[256:, rows_of(lax.rem(hi + 2, 4), 512)]
    for j in range(3):
        for half in range(2):
            gn_copy(j, half).wait_send()
            nm_copy(j, half).wait_send()


def store_kernel(so, sq, sk, sv, acc, nl, wl, out, grad_query, grad_key, grad_value, late, sem):
    copies = [
        pltpu.make_async_copy(held, placed, sem.at[i])
        for i, (held, placed) in enumerate(
            ((sq, grad_query), (sk, grad_key), (sv, grad_value), (so, out.at[pl.ds(0, 256), :]))
        )
    ]
    for copy in copies:
        copy.start()
    for n in range(4):
        cols = pl.ds(n * 512, 512)
        late[:, cols] = (acc[:, cols] + dot_nn(nl[...], wl[:, cols])).astype(BF16)
        copy = pltpu.make_async_copy(
            late.at[:, cols], out.at[pl.ds(256, 256), cols], sem.at[4 + n]
        )
        copy.start()
        copies.append(copy)
    for copy in copies:
        copy.wait()


def on_device(query, key, value, gain, w_out, d_out):
    tokens, width = query.shape
    hbm = pl.BlockSpec(memory_space=pl.ANY)
    vmem = pl.BlockSpec(memory_space=pltpu.VMEM)
    heads, nblocks = 4, 16
    tall = (tokens, width)
    squares = (nblocks, heads, HDIM, HDIM)
    dma = pltpu.SemaphoreType.DMA
    held = pl.pallas_call(
        kernel,
        out_shape=(
            pltpu.VMEM((256, d_out.shape[1]), BF16),
            pltpu.VMEM(tall, BF16),
            pltpu.VMEM(tall, BF16),
            pltpu.VMEM(tall, BF16),
            pltpu.VMEM((256, d_out.shape[1]), F32),
            pltpu.VMEM((256, width), BF16),
            pltpu.VMEM((width, d_out.shape[1]), BF16),
        ),
        in_specs=[hbm, hbm, hbm, vmem, hbm, hbm],
        out_specs=(vmem,) * 7,
        scratch_shapes=[
            pltpu.VMEM(tall, BF16),
            pltpu.VMEM(tall, BF16),
            pltpu.VMEM(tall, BF16),
            pltpu.VMEM(w_out.shape, BF16),
            pltpu.VMEM(d_out.shape, BF16),
            pltpu.VMEM((3, 512, width), BF16),
            pltpu.VMEM(tall, BF16),
            pltpu.VMEM(tall, BF16),
            pltpu.VMEM(d_out.shape, BF16),
            pltpu.VMEM(squares, BF16),
            pltpu.VMEM(squares, BF16),
            pltpu.VMEM(tall, BF16),
            pltpu.VMEM(squares, BF16),
            pltpu.VMEM(squares, F32),
            pltpu.VMEM(squares, F32),
            pltpu.VMEM(tall, F32),
            pltpu.VMEM(tall, F32),
            pltpu.VMEM((2, heads, HDIM, HDIM), F32),
            pltpu.VMEM((2, 512, HDIM), BF16),
            pltpu.VMEM((2, 8, 64, HDIM), BF16),
            pltpu.VMEM((2, 8, 64, HDIM), F32),
            pltpu.VMEM((2, 64, HDIM), BF16),
            pltpu.VMEM((2, 4, 64, HDIM), BF16),
            pltpu.VMEM((2, 8, 64, HDIM), BF16),
            pltpu.VMEM((2, 512, HDIM), BF16),
            dma((6,)), dma((4,)), dma((3, 2)), dma((3, 2)), dma((3, 2)), dma((3, 2)),
            dma((2, 7)), dma((2, 7)), dma((2, 3)), dma((2, 3)), dma((2, 7)), dma((2, 7)),
        ],
        compiler_params=pltpu.CompilerParams(
            collective_id=0, has_side_effects=True, vmem_limit_bytes=51 * 2**20
        ),
    )(query, key, value, gain, w_out, d_out)
    return pl.pallas_call(
        store_kernel,
        out_shape=tuple(
            jax.ShapeDtypeStruct(shape, BF16) for shape in (d_out.shape, tall, tall, tall)
        ),
        in_specs=[vmem] * 7,
        out_specs=(hbm,) * 4,
        scratch_shapes=[pltpu.VMEM((256, d_out.shape[1]), BF16), dma((8,))],
        compiler_params=pltpu.CompilerParams(vmem_limit_bytes=4 * 2**20),
    )(*held)


def solution(mesh):
    in_specs = (
        P("ctx", "head"), P("ctx", "head"), P("ctx", "head"), P("head"), P(),
        P(("ctx", "head"), None),
    )
    out_specs = (
        P(("ctx", "head"), None), P("ctx", "head"), P("ctx", "head"), P("ctx", "head"),
    )
    return jax.shard_map(
        on_device, mesh=mesh, in_specs=in_specs, out_specs=out_specs, check_vma=False
    )
```
